32 devices in a mesh: batch: 8 (over y, x, core), chan: 4 (over z).
Axes of the slice: x: 2, y: 2, z: 4, core: 2. Of those that a mesh axis runs over, the one named last changes fastest.
Arguments:
- images: bfloat16 [64, 14, 14, 4096], P('batch', None, None, 'chan'), may hold values from -12 to 12, as said below
- reduce_weight: bfloat16 [4096, 1024], P(None, 'chan'), may hold values from -0.09375 to 0.09375
- reduce_gain: float32 [1024], P('chan'), may hold values from 0.25 to 1.75
- reduce_bias: float32 [1024], P('chan'), may hold values from -0.5 to 0.5
- spatial_weight: bfloat16 [3, 3, 1024, 1024], P(None, None, None, 'chan'), may hold values from -0.0625 to 0.0625
- spatial_gain: float32 [1024], P('chan'), may hold values from 0.25 to 1.75
- spatial_bias: float32 [1024], P('chan'), may hold values from -0.5 to 0.5
- expand_weight: bfloat16 [1024, 4096], P(None, 'chan'), may hold values from -0.1875 to 0.1875
- expand_gain: float32 [4096], P('chan'), may hold values from 0.25 to 1.75
- expand_bias: float32 [4096], P('chan'), may hold values from -0.5 to 0.5
Outputs:
- block_out: bfloat16 [64, 14, 14, 4096], P('batch', None, None, 'chan')
The draws below stay inside these ranges and needn't reach their ends.
Inputs may be any that keep to these rules, and one draw needn't show every extreme that they name: In the images, the per-channel mean and scale differ from one block of 8 images to the next.
All inputs are finite; a program needn't handle non-finite values.
Results may differ from the reference program's by a relative error of at most 0.0047.
Values may be sent and summed in bfloat16 or wider, within the bound.
A program may use at most 128 MiB of HBM per device.

```python
import jax
import jax.numpy as jnp
from jax import lax

CIN = 4096
MID = 1024
SIDE = 14
IMG_DEV = 8
IMAGES = 64


def draw_images(key, part):
    k_offset, k_scale, k_base = jax.random.split(jax.random.fold_in(key, 11), 3)
    groups = IMAGES // IMG_DEV
    offset = jnp.clip(1.5 * jax.random.normal(k_offset, (groups, 1, 1, 1, CIN), jnp.float32), -3.0, 3.0)
    scales = jnp.exp(jax.random.uniform(k_scale, (groups, 1, 1, 1, CIN), jnp.float32, -0.693, 0.693))
    shape = (groups, IMG_DEV, SIDE, SIDE, CIN)
    base = jnp.clip(jax.random.normal(k_base, shape, jnp.float32), -4.0, 4.0)
    values = jnp.clip(offset + scales * base, -12.0, 12.0)
    return values.reshape(IMAGES, SIDE, SIDE, CIN).astype(jnp.bfloat16)


def steps_of(key, shape, shards, least, top_value):
    level, own = 1.0, jax.random.fold_in(key, 6)
    for position, shards_of in shards:
        steps = jnp.exp(jax.random.uniform(jax.random.fold_in(own, position), (shards_of,), jnp.float32, least / len(shards), top_value / len(shards)))
        level = level * jnp.repeat(steps, shape[position] // shards_of).reshape([-1 if axis == position else 1 for axis in range(len(shape))])
    return level


def normal_values(rng, shape, spread, reach, cuts=(), dtype=jnp.bfloat16):
    level = steps_of(rng, shape, cuts, -0.22, 0.18) if cuts else 1.0
    array = jax.random.normal(rng, shape, jnp.float32) * spread * level
    return jnp.minimum(jnp.maximum(array, -reach), reach).astype(dtype)


def setup_inputs(seed: int = 0) -> dict:
    streams_of = jax.random.split(jax.random.key(seed), 11)
    images = draw_images(jax.random.fold_in(streams_of[10], 71), 0)
    reduce_weight = normal_values(streams_of[1], (CIN, MID), CIN ** -0.5, 0.09375, ((1, 4),))
    reduce_gain = jnp.clip(1.0 + 0.15 * jax.random.normal(streams_of[2], (MID,), jnp.float32), 0.25, 1.75)
    reduce_bias = jnp.clip(jax.random.uniform(streams_of[3], (MID,), jnp.float32, -0.5, 0.5) * steps_of(streams_of[3], (MID,), ((0, 4),), -0.4, 0.0), -0.5, 0.5)
    spatial_weight = normal_values(streams_of[4], (3, 3, MID, MID), (9 * MID) ** -0.5, 0.0625, ((3, 4),))
    spatial_gain = jnp.clip(1.0 + 0.15 * jax.random.normal(streams_of[5], (MID,), jnp.float32), 0.25, 1.75)
    spatial_bias = jnp.clip(jax.random.uniform(streams_of[6], (MID,), jnp.float32, -0.5, 0.5) * steps_of(streams_of[6], (MID,), ((0, 4),), -0.4, 0.0), -0.5, 0.5)
    expand_weight = normal_values(streams_of[7], (MID, CIN), MID ** -0.5, 0.1875, ((1, 4),))
    expand_gain = jnp.clip(1.0 + 0.15 * jax.random.normal(streams_of[8], (CIN,), jnp.float32), 0.25, 1.75)
    expand_bias = jnp.clip(jax.random.uniform(streams_of[9], (CIN,), jnp.float32, -0.5, 0.5) * steps_of(streams_of[9], (CIN,), ((0, 4),), -0.4, 0.0), -0.5, 0.5)
    return dict(images=images, reduce_weight=reduce_weight, reduce_gain=reduce_gain, reduce_bias=reduce_bias, spatial_weight=spatial_weight, spatial_gain=spatial_gain, spatial_bias=spatial_bias, expand_weight=expand_weight, expand_gain=expand_gain, expand_bias=expand_bias)


eps = 0.001

def batch_norm(values, gain, bias):
    mean = lax.optimization_barrier(jnp.mean(values, axis=(0, 1, 2)))
    centred = values - mean
    var = lax.optimization_barrier(jnp.mean(centred * centred, axis=(0, 1, 2)))
    return centred * (gain / jnp.sqrt(var + eps)) + bias

def pointwise(maps, weight):
    flat = maps.reshape(-1, maps.shape[-1])
    out = jnp.dot(flat, weight, preferred_element_type=jnp.float32)
    return out.reshape(maps.shape[:-1] + (weight.shape[1],))

def reference(images, reduce_weight, reduce_gain, reduce_bias, spatial_weight, spatial_gain, spatial_bias, expand_weight, expand_gain, expand_bias):
    first = pointwise(images, reduce_weight)
    act_one = jnp.maximum(batch_norm(first, reduce_gain, reduce_bias), 0.0).astype(jnp.bfloat16)
    padded = jnp.pad(act_one, ((0, 0), (1, 1), (1, 1), (0, 0)))
    second = jnp.zeros(act_one.shape[:-1] + (spatial_weight.shape[3],), jnp.float32)
    for row_tap in range(3):
        for col_tap in range(3):
            window = padded[:, row_tap:row_tap + SIDE, col_tap:col_tap + SIDE, :]
            second = second + pointwise(window, spatial_weight[row_tap, col_tap])
    act_two = jnp.maximum(batch_norm(second, spatial_gain, spatial_bias), 0.0).astype(jnp.bfloat16)
    third = pointwise(act_two, expand_weight)
    summed = batch_norm(third, expand_gain, expand_bias) + images.astype(jnp.float32)
    return jnp.maximum(summed, 0.0).astype(jnp.bfloat16)
```

```python
import functools

import jax
import jax.numpy as jnp
from jax import lax
from jax.experimental import pallas as pl
from jax.experimental.pallas import tpu as pltpu
from jax.sharding import PartitionSpec as P

eps = 0.001
MESH = pl.DeviceIdType.MESH
LIMIT = 63 * 1024 * 1024


def remote(src, dst, send, recv, device):
    return pltpu.make_async_remote_copy(
        src_ref=src, dst_ref=dst, send_sem=send, recv_sem=recv,
        device_id=device, device_id_type=MESH,
    )


def greet(n, nb, z, b):
    barrier = pltpu.get_barrier_semaphore()
    for off in range(1, n):
        pl.semaphore_signal(
            barrier, inc=1, device_id={"chan": lax.rem(z + off, n)}, device_id_type=MESH
        )
    for off in range(1, nb):
        pl.semaphore_signal(
            barrier, inc=1, device_id={"batch": lax.rem(b + off, nb)}, device_id_type=MESH
        )
    pl.semaphore_wait(barrier, n + nb - 2)


def share_stats(nb, b, stat_in, send, recv):
    for off in range(1, nb):
        peer = lax.rem(b + off, nb)
        remote(
            stat_in.at[b], stat_in.at[b], send.at[off], recv.at[b], {"batch": peer}
        ).start()
    for off in range(1, nb):
        peer = lax.rem(b + off, nb)
        remote(
            stat_in.at[b], stat_in.at[peer], send.at[off], recv.at[peer], {"batch": peer}
        ).wait()


def combine(stats, local):
    nb = stats.shape[0]
    means = stats[..., 0:1, :]
    mean = jnp.sum(means, axis=0) / nb
    away = means - mean[None]
    spread = jnp.sum(stats[..., 1:2, :], axis=0) + local * jnp.sum(away * away, axis=0)
    return mean, spread / (local * nb)


def first_kernel(
    n, nb, parts, img_ref, w_ref, gb_ref, out_ref,
    wown, part, pre_in, suf_in, pre_out, suf_out, gb_in, shift, acc1, acc2, stat_in,
    w1_send, w1_recv, w2_send, w2_recv, w3_send, w3_recv, gb_send, gb_recv,
    pre_send, pre_recv, suf_send, suf_recv, st_send, st_recv,
):
    z, b = lax.axis_index("chan"), lax.axis_index("batch")
    depth = img_ref.shape[2]
    height = img_ref.shape[1]
    strip = depth // nb
    half = nb // 2
    chunks = n * parts
    partner = b + 1 - 2 * lax.rem(b, 2)
    parity = lax.rem(b, 2)
    greet(n, nb, z, b)

    def rows_of(who):
        return pl.ds(pl.multiple_of(who * strip, 16), strip)

    for off in range(1, n):
        to = lax.rem(z + off, n)
        src = w_ref.at[pl.ds(pl.multiple_of(to * depth + b * strip, 16), strip), :]
        remote(
            src, wown.at[z, rows_of(b), :], w1_send.at[off], w1_recv.at[z], {"chan": to}
        ).start()
    gb_in[z] = gb_ref[...]
    for off in range(1, n):
        to = lax.rem(z + off, n)
        remote(gb_ref, gb_in.at[z], gb_send.at[off], gb_recv.at[z], {"chan": to}).start()

    wown[z] = w_ref[pl.ds(pl.multiple_of(z * depth, 16), depth), :]

    @pl.when(z == 0)
    def _():
        pre_in[...] = jnp.zeros_like(pre_in)

    @pl.when(z == n - 1)
    def _():
        suf_in[...] = jnp.zeros_like(suf_in)

    def strip_copy(g, who, send, recv, device):
        ref = wown.at[g, rows_of(who), :]
        return remote(ref, ref, send, recv, device)

    for off in range(1, n):
        g = lax.rem(z + off, n)
        strip_copy(g, b, w1_send.at[0], w1_recv.at[g], {"chan": g}).wait_recv()
        for hop in range(1, half):
            peer = lax.rem(b + 2 * hop, nb)
            strip_copy(g, b, w2_send.at[off, hop], w2_recv.at[g, b], {"batch": peer}).start()
        strip_copy(g, b, w3_send.at[off, 0], w3_recv.at[g, b], {"batch": partner}).start()
    for off in range(1, n):
        g = lax.rem(z + off, n)
        for hop in range(1, half):
            peer = lax.rem(b + 2 * hop, nb)
            strip_copy(g, peer, w2_send.at[0, 0], w2_recv.at[g, peer], {"batch": peer}).wait_recv()
            strip_copy(
                g, peer, w3_send.at[off, hop], w3_recv.at[g, peer], {"batch": partner}
            ).start()
    for off in range(1, n):
        g = lax.rem(z + off, n)
        for hop in range(half):
            who = 2 * hop + 1 - parity
            strip_copy(g, who, w3_send.at[0, 0], w3_recv.at[g, who], {"batch": partner}).wait_recv()

    def right_copy(k):
        return remote(
            pre_out.at[k], pre_in.at[k], pre_send.at[k], pre_recv.at[k],
            {"chan": lax.rem(z + 1, n)},
        )

    def left_copy(k):
        return remote(
            suf_out.at[k], suf_in.at[k], suf_send.at[k], suf_recv.at[k],
            {"chan": lax.rem(z + n - 1, n)},
        )

    def step(s, carry):
        @pl.when(s < chunks)
        def _():
            g, r = lax.div(s, parts), lax.rem(s, parts)
            part[s] = jnp.dot(img_ref[r], wown[g], preferred_element_type=jnp.float32)

        kp = s - z

        @pl.when(jnp.logical_and(kp >= 0, kp < chunks))
        def _():
            @pl.when(z > 0)
            def _():
                right_copy(kp).wait_recv()

            @pl.when(z < n - 1)
            def _():
                pre_out[kp] = (part[kp] + pre_in[kp].astype(jnp.float32)).astype(jnp.bfloat16)
                right_copy(kp).start()

        ks = s - (n - 1 - z)

        @pl.when(jnp.logical_and(ks >= 0, ks < chunks))
        def _():
            @pl.when(z < n - 1)
            def _():
                left_copy(ks).wait_recv()

            @pl.when(z > 0)
            def _():
                suf_out[ks] = (part[ks] + suf_in[ks].astype(jnp.float32)).astype(jnp.bfloat16)
                left_copy(ks).start()

        kf = s - jnp.maximum(z, n - 1 - z)

        @pl.when(jnp.logical_and(kf >= 0, kf < chunks))
        def _():
            g, r = lax.div(kf, parts), lax.rem(kf, parts)
            value = (
                part[kf] + pre_in[kf].astype(jnp.float32) + suf_in[kf].astype(jnp.float32)
            )
            part[kf] = value

            @pl.when(r == 0)
            def _():
                shift[g] = jnp.sum(value, axis=0, keepdims=True) / height
                acc1[g] = jnp.zeros_like(acc1[g])
                acc2[g] = jnp.zeros_like(acc2[g])

            moved = value - shift[g]
            acc1[g] += jnp.sum(moved, axis=0, keepdims=True)
            acc2[g] += jnp.sum(moved * moved, axis=0, keepdims=True)

        return carry

    lax.fori_loop(0, chunks + n - 1, step, 0)

    local = height * parts
    extra = acc1[...] / local
    stat_in[b, :, 0:1, :] = shift[...] + extra
    stat_in[b, :, 1:2, :] = acc2[...] - acc1[...] * extra
    share_stats(nb, b, stat_in, st_send, st_recv)
    for off in range(1, n):
        g = lax.rem(z + off, n)
        remote(gb_ref, gb_in.at[g], gb_send.at[off], gb_recv.at[g], {"chan": g}).wait()
    mean, var = combine(stat_in[...], local)
    scale = gb_in[:, 0:1, :] / jnp.sqrt(var + eps)
    bias = gb_in[:, 1:2, :]
    width = part.shape[2]

    def finish(r, carry):
        for g in range(n):
            value = (part[g * parts + r] - mean[g]) * scale[g] + bias[g]
            out_ref[r, :, g * width : (g + 1) * width] = jnp.maximum(value, 0.0).astype(
                jnp.bfloat16
            )
        return carry

    lax.fori_loop(0, parts, finish, 0)

    for off in range(1, n):
        to = lax.rem(z + off, n)
        src = w_ref.at[pl.ds(pl.multiple_of(to * depth + b * strip, 16), strip), :]
        remote(
            src, wown.at[z, rows_of(b), :], w1_send.at[off], w1_recv.at[z], {"chan": to}
        ).wait_send()
        g = to
        for hop in range(1, half):
            peer = lax.rem(b + 2 * hop, nb)
            strip_copy(g, b, w2_send.at[off, hop], w2_recv.at[g, b], {"batch": peer}).wait_send()
        for hop in range(half):
            peer = lax.rem(b + 2 * hop, nb)
            strip_copy(
                g, peer, w3_send.at[off, hop], w3_recv.at[g, peer], {"batch": partner}
            ).wait_send()

    def drain(k, carry):
        @pl.when(z < n - 1)
        def _():
            right_copy(k).wait_send()

        @pl.when(z > 0)
        def _():
            left_copy(k).wait_send()

        return carry

    lax.fori_loop(0, chunks, drain, 0)


def third_kernel(
    n, nb, sec_ref, gb_ref, w_ref, gain_ref, out_ref, norm_ref,
    act, stat2, stat3,
    right_send, left_send, recv, s2_send, s2_recv, s3_send, s3_recv,
):
    z, b = lax.axis_index("chan"), lax.axis_index("batch")
    parts, height, width = sec_ref.shape
    local = parts * height
    greet(n, nb, z, b)
    values = sec_ref[...]
    own = jnp.sum(jnp.sum(values, axis=0), axis=0, keepdims=True) / local
    away = values - own[None]
    stat2[b, 0:1, :] = own
    stat2[b, 1:2, :] = jnp.sum(jnp.sum(away * away, axis=0), axis=0, keepdims=True)
    share_stats(nb, b, stat2, s2_send, s2_recv)
    mean, var = combine(stat2[...], local)
    scale = gb_ref[0:1, :] / jnp.sqrt(var + eps)
    bias = gb_ref[1:2, :]

    def right_copy(g, r):
        ref = act.at[g, r]
        return remote(
            ref, ref, right_send.at[g, r], recv.at[g, r], {"chan": lax.rem(z + 1, n)}
        )

    def left_copy(g, r):
        ref = act.at[g, r]
        return remote(
            ref, ref, left_send.at[g, r], recv.at[g, r], {"chan": lax.rem(z + n - 1, n)}
        )

    def rows_of(g):
        return pl.ds(pl.multiple_of(g * width, 128), width)

    def begin(r, carry):
        value = (sec_ref[r] - mean) * scale + bias
        act[z, r] = jnp.maximum(value, 0.0).astype(jnp.bfloat16)

        @pl.when(z < n - 1)
        def _():
            right_copy(z, r).start()

        @pl.when(z > 0)
        def _():
            left_copy(z, r).start()

        out_ref[r] = jnp.dot(act[z, r], w_ref[rows_of(z), :], preferred_element_type=jnp.float32)
        return carry

    lax.fori_loop(0, parts, begin, 0)

    def relay(s, carry):
        d, r = lax.div(s, parts) + 1, lax.rem(s, parts)
        g = z - d

        @pl.when(g >= 0)
        def _():
            right_copy(g, r).wait_recv()

            @pl.when(z < n - 1)
            def _():
                right_copy(g, r).start()

            out_ref[r] += jnp.dot(
                act[g, r], w_ref[rows_of(g), :], preferred_element_type=jnp.float32
            )

        h = z + d

        @pl.when(h < n)
        def _():
            left_copy(h, r).wait_recv()

            @pl.when(z > 0)
            def _():
                left_copy(h, r).start()

            out_ref[r] += jnp.dot(
                act[h, r], w_ref[rows_of(h), :], preferred_element_type=jnp.float32
            )

        return carry

    lax.fori_loop(0, parts * (n - 1), relay, 0)

    def add(r, carry):
        return carry + jnp.sum(out_ref[r], axis=0, keepdims=True)

    zero = jnp.zeros((1, out_ref.shape[2]), jnp.float32)
    own3 = lax.fori_loop(0, parts, add, zero) / local

    def add_square(r, carry):
        away = out_ref[r] - own3
        return carry + jnp.sum(away * away, axis=0, keepdims=True)

    stat3[b, 0:1, :] = own3
    stat3[b, 1:2, :] = lax.fori_loop(0, parts, add_square, zero)
    share_stats(nb, b, stat3, s3_send, s3_recv)
    mean3, var3 = combine(stat3[...], local)
    norm_ref[0:1, :] = mean3
    norm_ref[1:2, :] = gain_ref[...] / jnp.sqrt(var3 + eps)

    def drain(s, carry):
        g, r = lax.div(s, parts), lax.rem(s, parts)

        @pl.when(jnp.logical_and(z < n - 1, g <= z))
        def _():
            right_copy(g, r).wait_send()

        @pl.when(jnp.logical_and(z > 0, g >= z))
        def _():
            left_copy(g, r).wait_send()

        return carry

    lax.fori_loop(0, n * parts, drain, 0)


def parts_of(rows):
    for parts in (7, 4, 2):
        if rows % (parts * 16) == 0:
            return parts
    return 1


def body(
    images,
    reduce_weight,
    reduce_gain,
    reduce_bias,
    spatial_weight,
    spatial_gain,
    spatial_bias,
    expand_weight,
    expand_gain,
    expand_bias,
):
    imgs, side = (images.shape[0], images.shape[1])
    rows = imgs * side * side
    n, nb = lax.axis_size("chan"), lax.axis_size("batch")
    mid_local = reduce_weight.shape[1]
    mid = mid_local * n
    depth = images.shape[3]
    out_local = expand_weight.shape[1]
    parts = parts_of(rows)
    height = rows // parts
    chunks = n * parts
    dma, f32, bf16 = pltpu.SemaphoreType.DMA, jnp.float32, jnp.bfloat16
    vmem = pl.BlockSpec(memory_space=pltpu.VMEM)
    flat = images.reshape(parts, height, depth)
    act_one = pl.pallas_call(
        functools.partial(first_kernel, n, nb, parts),
        out_shape=jax.ShapeDtypeStruct((parts, height, mid), bf16),
        in_specs=[vmem] * 3,
        out_specs=vmem,
        scratch_shapes=[
            pltpu.VMEM((n, depth, mid_local), bf16),
            pltpu.VMEM((chunks, height, mid_local), f32),
        ]
        + [pltpu.VMEM((chunks, height, mid_local), bf16)] * 4
        + [pltpu.VMEM((n, 2, mid_local), f32)]
        + [pltpu.VMEM((n, 1, mid_local), f32)] * 3
        + [pltpu.VMEM((nb, n, 2, mid_local), f32)]
        + [dma((n,)), dma((n,)), dma((n, nb // 2)), dma((n, nb)), dma((n, nb // 2)), dma((n, nb))]
        + [dma((n,)), dma((n,))]
        + [dma((chunks,))] * 4
        + [dma((nb,)), dma((nb,))],
        compiler_params=pltpu.CompilerParams(
            collective_id=0, has_side_effects=True, vmem_limit_bytes=LIMIT
        ),
        name="first",
    )(flat, reduce_weight, jnp.stack([reduce_gain, reduce_bias]))
    second = lax.conv_general_dilated(
        act_one.reshape(imgs, side, side, mid),
        spatial_weight,
        (1, 1),
        ((1, 1), (1, 1)),
        dimension_numbers=("NHWC", "HWIO", "NHWC"),
        preferred_element_type=f32,
    )
    third, norm = pl.pallas_call(
        functools.partial(third_kernel, n, nb),
        out_shape=(
            jax.ShapeDtypeStruct((parts, height, out_local), f32),
            jax.ShapeDtypeStruct((2, out_local), f32),
        ),
        in_specs=[vmem] * 4,
        out_specs=(vmem, vmem),
        scratch_shapes=[
            pltpu.VMEM((n, parts, height, mid_local), bf16),
            pltpu.VMEM((nb, 2, mid_local), f32),
            pltpu.VMEM((nb, 2, out_local), f32),
        ]
        + [dma((n, parts))] * 3
        + [dma((nb,))] * 4,
        compiler_params=pltpu.CompilerParams(
            collective_id=1, has_side_effects=True, vmem_limit_bytes=LIMIT
        ),
        name="third",
    )(
        second.reshape(parts, height, mid_local),
        jnp.stack([spatial_gain, spatial_bias]),
        expand_weight,
        expand_gain[None, :],
    )
    normed = (third.reshape(rows, out_local) - norm[0]) * norm[1] + expand_bias
    summed = normed + images.reshape(rows, out_local).astype(f32)
    return jnp.maximum(summed, 0.0).astype(bf16).reshape(imgs, side, side, out_local)


def solution(mesh):
    in_specs = (
        P("batch", None, None, "chan"),
        P(None, "chan"),
        P("chan"),
        P("chan"),
        P(None, None, None, "chan"),
        P("chan"),
        P("chan"),
        P(None, "chan"),
        P("chan"),
        P("chan"),
    )
    out_specs = P("batch", None, None, "chan")
    return jax.shard_map(body, mesh=mesh, in_specs=in_specs, out_specs=out_specs, check_vma=False)
```

```python
import functools

import jax
import jax.numpy as jnp
from jax import lax
from jax.experimental import pallas as pl
from jax.experimental.pallas import tpu as pltpu
from jax.sharding import PartitionSpec as P

eps = 0.001
MESH = pl.DeviceIdType.MESH
LIMIT = 63 * 1024 * 1024
SKEW = 3


def remote(src, dst, send, recv, device):
    return pltpu.make_async_remote_copy(
        src_ref=src, dst_ref=dst, send_sem=send, recv_sem=recv,
        device_id=device, device_id_type=MESH,
    )


def greet(n, nb, z, b):
    barrier = pltpu.get_barrier_semaphore()
    for off in range(1, n):
        pl.semaphore_signal(
            barrier, inc=1, device_id={"chan": lax.rem(z + off, n)}, device_id_type=MESH
        )
    for off in range(1, nb):
        pl.semaphore_signal(
            barrier, inc=1, device_id={"batch": lax.rem(b + off, nb)}, device_id_type=MESH
        )
    pl.semaphore_wait(barrier, n + nb - 2)


def share_stats(nb, b, stat_in, send, recv):
    for off in range(1, nb):
        peer = lax.rem(b + off, nb)
        remote(
            stat_in.at[b], stat_in.at[b], send.at[off], recv.at[b], {"batch": peer}
        ).start()
    for off in range(1, nb):
        peer = lax.rem(b + off, nb)
        remote(
            stat_in.at[b], stat_in.at[peer], send.at[off], recv.at[peer], {"batch": peer}
        ).wait()


def combine(stats, local):
    nb = stats.shape[0]
    means = stats[..., 0:1, :]
    mean = jnp.sum(means, axis=0) / nb
    away = means - mean[None]
    spread = jnp.sum(stats[..., 1:2, :], axis=0) + local * jnp.sum(away * away, axis=0)
    return mean, spread / (local * nb)


def first_kernel(
    n, nb, parts, img_ref, w_ref, gb_ref, out_ref,
    wown, part, pre_in, suf_in, pre_out, suf_out, gb_in, shift, acc1, acc2, stat_in,
    w1_send, w1_recv, w2_send, w2_recv, w3_send, w3_recv, gb_send, gb_recv,
    pre_send, pre_recv, suf_send, suf_recv, st_send, st_recv,
):
    z, b = lax.axis_index("chan"), lax.axis_index("batch")
    depth = img_ref.shape[2]
    height = img_ref.shape[1]
    strip = depth // nb
    half = nb // 2
    chunks = n * parts
    partner = b + 1 - 2 * lax.rem(b, 2)
    parity = lax.rem(b, 2)
    greet(n, nb, z, b)

    def rows_of(who):
        return pl.ds(pl.multiple_of(who * strip, 16), strip)

    for off in range(1, n):
        to = lax.rem(z + off, n)
        src = w_ref.at[pl.ds(pl.multiple_of(to * depth + b * strip, 16), strip), :]
        remote(
            src, wown.at[z, rows_of(b), :], w1_send.at[off], w1_recv.at[z], {"chan": to}
        ).start()
    gb_in[z] = gb_ref[...]
    for off in range(1, n):
        to = lax.rem(z + off, n)
        remote(gb_ref, gb_in.at[z], gb_send.at[off], gb_recv.at[z], {"chan": to}).start()

    wown[z] = w_ref[pl.ds(pl.multiple_of(z * depth, 16), depth), :]

    @pl.when(z == 0)
    def _():
        pre_in[...] = jnp.zeros_like(pre_in)

    @pl.when(z == n - 1)
    def _():
        suf_in[...] = jnp.zeros_like(suf_in)

    def strip_copy(g, who, send, recv, device):
        ref = wown.at[g, rows_of(who), :]
        return remote(ref, ref, send, recv, device)

    for g in range(n):

        @pl.when(z != g)
        def _():
            strip_copy(g, b, w1_send.at[0], w1_recv.at[g], {"chan": g}).wait_recv()
            for hop in range(1, half):
                peer = lax.rem(b + 2 * hop, nb)
                strip_copy(g, b, w2_send.at[g, hop], w2_recv.at[g, b], {"batch": peer}).start()
            strip_copy(g, b, w3_send.at[g, 0], w3_recv.at[g, b], {"batch": partner}).start()

    def forward(g):
        @pl.when(z != g)
        def _():
            for hop in range(1, half):
                peer = lax.rem(b + 2 * hop, nb)
                strip_copy(
                    g, peer, w2_send.at[g, 0], w2_recv.at[g, peer], {"batch": peer}
                ).wait_recv()
                strip_copy(
                    g, peer, w3_send.at[g, hop], w3_recv.at[g, peer], {"batch": partner}
                ).start()

    def complete(g):
        @pl.when(z != g)
        def _():
            for hop in range(half):
                who = 2 * hop + 1 - parity
                strip_copy(
                    g, who, w3_send.at[g, 0], w3_recv.at[g, who], {"batch": partner}
                ).wait_recv()

    forward(0)

    def right_copy(k):
        return remote(
            pre_out.at[k], pre_in.at[k], pre_send.at[k], pre_recv.at[k],
            {"chan": lax.rem(z + 1, n)},
        )

    def left_copy(k):
        return remote(
            suf_out.at[k], suf_in.at[k], suf_send.at[k], suf_recv.at[k],
            {"chan": lax.rem(z + n - 1, n)},
        )

    def step(s, carry):
        @pl.when(s < chunks)
        def _():
            g, r = lax.div(s, parts), lax.rem(s, parts)

            @pl.when(r == 0)
            def _():
                complete(g)

            @pl.when(jnp.logical_and(r == parts // 2, g < n - 1))
            def _():
                forward(g + 1)

            part[s] = jnp.dot(img_ref[r], wown[g], preferred_element_type=jnp.float32)

        kp = s - SKEW * z

        @pl.when(jnp.logical_and(kp >= 0, kp < chunks))
        def _():
            @pl.when(z > 0)
            def _():
                right_copy(kp).wait_recv()

            @pl.when(z < n - 1)
            def _():
                pre_out[kp] = (part[kp] + pre_in[kp].astype(jnp.float32)).astype(jnp.bfloat16)
                right_copy(kp).start()

        ks = s - SKEW * (n - 1 - z)

        @pl.when(jnp.logical_and(ks >= 0, ks < chunks))
        def _():
            @pl.when(z < n - 1)
            def _():
                left_copy(ks).wait_recv()

            @pl.when(z > 0)
            def _():
                suf_out[ks] = (part[ks] + suf_in[ks].astype(jnp.float32)).astype(jnp.bfloat16)
                left_copy(ks).start()

        kf = s - SKEW * jnp.maximum(z, n - 1 - z)

        @pl.when(jnp.logical_and(kf >= 0, kf < chunks))
        def _():
            g, r = lax.div(kf, parts), lax.rem(kf, parts)
            value = (
                part[kf] + pre_in[kf].astype(jnp.float32) + suf_in[kf].astype(jnp.float32)
            )
            part[kf] = value

            @pl.when(r == 0)
            def _():
                shift[g] = jnp.sum(value, axis=0, keepdims=True) / height
                acc1[g] = jnp.zeros_like(acc1[g])
                acc2[g] = jnp.zeros_like(acc2[g])

            moved = value - shift[g]
            acc1[g] += jnp.sum(moved, axis=0, keepdims=True)
            acc2[g] += jnp.sum(moved * moved, axis=0, keepdims=True)

        return carry

    lax.fori_loop(0, chunks + SKEW * (n - 1), step, 0)

    local = height * parts
    extra = acc1[...] / local
    stat_in[b, :, 0:1, :] = shift[...] + extra
    stat_in[b, :, 1:2, :] = acc2[...] - acc1[...] * extra
    share_stats(nb, b, stat_in, st_send, st_recv)
    for off in range(1, n):
        g = lax.rem(z + off, n)
        remote(gb_ref, gb_in.at[g], gb_send.at[off], gb_recv.at[g], {"chan": g}).wait()
    mean, var = combine(stat_in[...], local)
    scale = gb_in[:, 0:1, :] / jnp.sqrt(var + eps)
    bias = gb_in[:, 1:2, :]
    width = part.shape[2]

    def finish(r, carry):
        for g in range(n):
            value = (part[g * parts + r] - mean[g]) * scale[g] + bias[g]
            out_ref[r, :, g * width : (g + 1) * width] = jnp.maximum(value, 0.0).astype(
                jnp.bfloat16
            )
        return carry

    lax.fori_loop(0, parts, finish, 0)

    for off in range(1, n):
        to = lax.rem(z + off, n)
        src = w_ref.at[pl.ds(pl.multiple_of(to * depth + b * strip, 16), strip), :]
        remote(
            src, wown.at[z, rows_of(b), :], w1_send.at[off], w1_recv.at[z], {"chan": to}
        ).wait_send()
        g = to
        for hop in range(1, half):
            peer = lax.rem(b + 2 * hop, nb)
            strip_copy(g, b, w2_send.at[g, hop], w2_recv.at[g, b], {"batch": peer}).wait_send()
        for hop in range(half):
            peer = lax.rem(b + 2 * hop, nb)
            strip_copy(
                g, peer, w3_send.at[g, hop], w3_recv.at[g, peer], {"batch": partner}
            ).wait_send()

    def drain(k, carry):
        @pl.when(z < n - 1)
        def _():
            right_copy(k).wait_send()

        @pl.when(z > 0)
        def _():
            left_copy(k).wait_send()

        return carry

    lax.fori_loop(0, chunks, drain, 0)


def third_kernel(
    n, nb, sec_ref, gb_ref, w_ref, gain_ref, out_ref, norm_ref,
    act, stat2, stat3,
    right_send, left_send, recv, s2_send, s2_recv, s3_send, s3_recv,
):
    z, b = lax.axis_index("chan"), lax.axis_index("batch")
    parts, height, width = sec_ref.shape
    local = parts * height
    greet(n, nb, z, b)
    values = sec_ref[...]
    own = jnp.sum(jnp.sum(values, axis=0), axis=0, keepdims=True) / local
    away = values - own[None]
    stat2[b, 0:1, :] = own
    stat2[b, 1:2, :] = jnp.sum(jnp.sum(away * away, axis=0), axis=0, keepdims=True)
    share_stats(nb, b, stat2, s2_send, s2_recv)
    mean, var = combine(stat2[...], local)
    scale = gb_ref[0:1, :] / jnp.sqrt(var + eps)
    bias = gb_ref[1:2, :]

    def right_copy(g, r):
        ref = act.at[g, r]
        return remote(
            ref, ref, right_send.at[g, r], recv.at[g, r], {"chan": lax.rem(z + 1, n)}
        )

    def left_copy(g, r):
        ref = act.at[g, r]
        return remote(
            ref, ref, left_send.at[g, r], recv.at[g, r], {"chan": lax.rem(z + n - 1, n)}
        )

    def rows_of(g):
        return pl.ds(pl.multiple_of(g * width, 128), width)

    def begin(r, carry):
        value = (sec_ref[r] - mean) * scale + bias
        act[z, r] = jnp.maximum(value, 0.0).astype(jnp.bfloat16)

        @pl.when(z < n - 1)
        def _():
            right_copy(z, r).start()

        @pl.when(z > 0)
        def _():
            left_copy(z, r).start()

        out_ref[r] = jnp.dot(act[z, r], w_ref[rows_of(z), :], preferred_element_type=jnp.float32)
        return carry

    lax.fori_loop(0, parts, begin, 0)

    def relay(s, carry):
        d, r = lax.div(s, parts) + 1, lax.rem(s, parts)
        g = z - d

        @pl.when(g >= 0)
        def _():
            right_copy(g, r).wait_recv()

            @pl.when(z < n - 1)
            def _():
                right_copy(g, r).start()

            out_ref[r] += jnp.dot(
                act[g, r], w_ref[rows_of(g), :], preferred_element_type=jnp.float32
            )

        h = z + d

        @pl.when(h < n)
        def _():
            left_copy(h, r).wait_recv()

            @pl.when(z > 0)
            def _():
                left_copy(h, r).start()

            out_ref[r] += jnp.dot(
                act[h, r], w_ref[rows_of(h), :], preferred_element_type=jnp.float32
            )

        return carry

    lax.fori_loop(0, parts * (n - 1), relay, 0)

    def add(r, carry):
        return carry + jnp.sum(out_ref[r], axis=0, keepdims=True)

    zero = jnp.zeros((1, out_ref.shape[2]), jnp.float32)
    own3 = lax.fori_loop(0, parts, add, zero) / local

    def add_square(r, carry):
        away = out_ref[r] - own3
        return carry + jnp.sum(away * away, axis=0, keepdims=True)

    stat3[b, 0:1, :] = own3
    stat3[b, 1:2, :] = lax.fori_loop(0, parts, add_square, zero)
    share_stats(nb, b, stat3, s3_send, s3_recv)
    mean3, var3 = combine(stat3[...], local)
    norm_ref[0:1, :] = mean3
    norm_ref[1:2, :] = gain_ref[...] / jnp.sqrt(var3 + eps)

    def drain(s, carry):
        g, r = lax.div(s, parts), lax.rem(s, parts)

        @pl.when(jnp.logical_and(z < n - 1, g <= z))
        def _():
            right_copy(g, r).wait_send()

        @pl.when(jnp.logical_and(z > 0, g >= z))
        def _():
            left_copy(g, r).wait_send()

        return carry

    lax.fori_loop(0, n * parts, drain, 0)


def body(
    images,
    reduce_weight,
    reduce_gain,
    reduce_bias,
    spatial_weight,
    spatial_gain,
    spatial_bias,
    expand_weight,
    expand_gain,
    expand_bias,
):
    imgs, side = (images.shape[0], images.shape[1])
    n, nb = lax.axis_size("chan"), lax.axis_size("batch")
    mid_local = reduce_weight.shape[1]
    mid = mid_local * n
    depth = images.shape[3]
    out_local = expand_weight.shape[1]
    parts, height = side, side * imgs
    chunks = n * parts
    dma, f32, bf16 = pltpu.SemaphoreType.DMA, jnp.float32, jnp.bfloat16
    vmem = pl.BlockSpec(memory_space=pltpu.VMEM)
    flat = images.transpose(1, 2, 0, 3).reshape(parts, height, depth)
    act_one = pl.pallas_call(
        functools.partial(first_kernel, n, nb, parts),
        out_shape=jax.ShapeDtypeStruct((parts, height, mid), bf16),
        in_specs=[vmem] * 3,
        out_specs=vmem,
        scratch_shapes=[
            pltpu.VMEM((n, depth, mid_local), bf16),
            pltpu.VMEM((chunks, height, mid_local), f32),
        ]
        + [pltpu.VMEM((chunks, height, mid_local), bf16)] * 4
        + [pltpu.VMEM((n, 2, mid_local), f32)]
        + [pltpu.VMEM((n, 1, mid_local), f32)] * 3
        + [pltpu.VMEM((nb, n, 2, mid_local), f32)]
        + [dma((n,)), dma((n,)), dma((n, nb // 2)), dma((n, nb)), dma((n, nb // 2)), dma((n, nb))]
        + [dma((n,)), dma((n,))]
        + [dma((chunks,))] * 4
        + [dma((nb,)), dma((nb,))],
        compiler_params=pltpu.CompilerParams(
            collective_id=0, has_side_effects=True, vmem_limit_bytes=LIMIT
        ),
        name="first",
    )(flat, reduce_weight, jnp.stack([reduce_gain, reduce_bias]))
    second = lax.conv_general_dilated(
        act_one.reshape(side, side, imgs, mid),
        spatial_weight,
        (1, 1),
        ((1, 1), (1, 1)),
        dimension_numbers=("HWNC", "HWIO", "HWNC"),
        preferred_element_type=f32,
    )
    third, norm = pl.pallas_call(
        functools.partial(third_kernel, n, nb),
        out_shape=(
            jax.ShapeDtypeStruct((parts, height, out_local), f32),
            jax.ShapeDtypeStruct((2, out_local), f32),
        ),
        in_specs=[vmem] * 4,
        out_specs=(vmem, vmem),
        scratch_shapes=[
            pltpu.VMEM((n, parts, height, mid_local), bf16),
            pltpu.VMEM((nb, 2, mid_local), f32),
            pltpu.VMEM((nb, 2, out_local), f32),
        ]
        + [dma((n, parts))] * 3
        + [dma((nb,))] * 4,
        compiler_params=pltpu.CompilerParams(
            collective_id=1, has_side_effects=True, vmem_limit_bytes=LIMIT
        ),
        name="third",
    )(
        second.reshape(parts, height, mid_local),
        jnp.stack([spatial_gain, spatial_bias]),
        expand_weight,
        expand_gain[None, :],
    )
    normed = (third - norm[0]) * norm[1] + expand_bias
    out = jnp.maximum(normed + flat.astype(f32), 0.0).astype(bf16)
    return out.reshape(side, side, imgs, out_local).transpose(2, 0, 1, 3)


def solution(mesh):
    in_specs = (
        P("batch", None, None, "chan"),
        P(None, "chan"),
        P("chan"),
        P("chan"),
        P(None, None, None, "chan"),
        P("chan"),
        P("chan"),
        P(None, "chan"),
        P("chan"),
        P("chan"),
    )
    out_specs = P("batch", None, None, "chan")
    return jax.shard_map(body, mesh=mesh, in_specs=in_specs, out_specs=out_specs, check_vma=False)
```

```python
import functools

import jax
import jax.numpy as jnp
from jax import lax
from jax.experimental import pallas as pl
from jax.experimental.pallas import tpu as pltpu
from jax.sharding import PartitionSpec as P

eps = 0.001
MESH = pl.DeviceIdType.MESH
LIMIT = 63 * 1024 * 1024
SKEW = 3


def remote(src, dst, send, recv, device):
    return pltpu.make_async_remote_copy(
        src_ref=src, dst_ref=dst, send_sem=send, recv_sem=recv,
        device_id=device, device_id_type=MESH,
    )


def greet(n, nb, z, b):
    barrier = pltpu.get_barrier_semaphore()
    for off in range(1, n):
        pl.semaphore_signal(
            barrier, inc=1, device_id={"chan": lax.rem(z + off, n)}, device_id_type=MESH
        )
    for off in range(1, nb):
        pl.semaphore_signal(
            barrier, inc=1, device_id={"batch": lax.rem(b + off, nb)}, device_id_type=MESH
        )
    pl.semaphore_wait(barrier, n + nb - 2)


def share_stats(nb, b, stat_in, send, recv):
    for off in range(1, nb):
        peer = lax.rem(b + off, nb)
        remote(
            stat_in.at[b], stat_in.at[b], send.at[off], recv.at[b], {"batch": peer}
        ).start()
    for off in range(1, nb):
        peer = lax.rem(b + off, nb)
        remote(
            stat_in.at[b], stat_in.at[peer], send.at[off], recv.at[peer], {"batch": peer}
        ).wait()


def combine(stats, local):
    nb = stats.shape[0]
    means = stats[..., 0:1, :]
    mean = jnp.sum(means, axis=0) / nb
    away = means - mean[None]
    spread = jnp.sum(stats[..., 1:2, :], axis=0) + local * jnp.sum(away * away, axis=0)
    return mean, spread / (local * nb)


def first_kernel(
    n, nb, parts, img_ref, w_ref, gb_ref, out_ref,
    wown, part, pre_in, suf_in, pre_out, suf_out, gb_in, shift, acc1, acc2, stat_in,
    w1_send, w1_recv, w2_send, w2_recv, w3_send, w3_recv, gb_send, gb_recv,
    pre_send, pre_recv, suf_send, suf_recv, st_send, st_recv,
):
    z, b = lax.axis_index("chan"), lax.axis_index("batch")
    depth = img_ref.shape[2]
    height = img_ref.shape[1]
    strip = depth // nb
    half = nb // 2
    chunks = n * parts
    partner = b + 1 - 2 * lax.rem(b, 2)
    parity = lax.rem(b, 2)
    greet(n, nb, z, b)

    def rows_of(who):
        return pl.ds(pl.multiple_of(who * strip, 16), strip)

    for off in range(1, n):
        to = lax.rem(z + off, n)
        src = w_ref.at[pl.ds(pl.multiple_of(to * depth + b * strip, 16), strip), :]
        remote(
            src, wown.at[z, rows_of(b), :], w1_send.at[off], w1_recv.at[z], {"chan": to}
        ).start()
    gb_in[z] = gb_ref[...]
    for off in range(1, n):
        to = lax.rem(z + off, n)
        remote(gb_ref, gb_in.at[z], gb_send.at[off], gb_recv.at[z], {"chan": to}).start()

    wown[z] = w_ref[pl.ds(pl.multiple_of(z * depth, 16), depth), :]

    @pl.when(z == 0)
    def _():
        pre_in[...] = jnp.zeros_like(pre_in)

    @pl.when(z == n - 1)
    def _():
        suf_in[...] = jnp.zeros_like(suf_in)

    def strip_copy(g, who, send, recv, device):
        ref = wown.at[g, rows_of(who), :]
        return remote(ref, ref, send, recv, device)

    for g in range(n):

        @pl.when(z != g)
        def _():
            strip_copy(g, b, w1_send.at[0], w1_recv.at[g], {"chan": g}).wait_recv()
            for hop in range(1, half):
                peer = lax.rem(b + 2 * hop, nb)
                strip_copy(g, b, w2_send.at[g, hop], w2_recv.at[g, b], {"batch": peer}).start()
            strip_copy(g, b, w3_send.at[g, 0], w3_recv.at[g, b], {"batch": partner}).start()

    def forward(g):
        @pl.when(z != g)
        def _():
            for hop in range(1, half):
                peer = lax.rem(b + 2 * hop, nb)
                strip_copy(
                    g, peer, w2_send.at[g, 0], w2_recv.at[g, peer], {"batch": peer}
                ).wait_recv()
                strip_copy(
                    g, peer, w3_send.at[g, hop], w3_recv.at[g, peer], {"batch": partner}
                ).start()

    def complete(g):
        @pl.when(z != g)
        def _():
            for hop in range(half):
                who = 2 * hop + 1 - parity
                strip_copy(
                    g, who, w3_send.at[g, 0], w3_recv.at[g, who], {"batch": partner}
                ).wait_recv()

    forward(0)

    def right_copy(k):
        return remote(
            pre_out.at[k], pre_in.at[k], pre_send.at[k], pre_recv.at[k],
            {"chan": lax.rem(z + 1, n)},
        )

    def left_copy(k):
        return remote(
            suf_out.at[k], suf_in.at[k], suf_send.at[k], suf_recv.at[k],
            {"chan": lax.rem(z + n - 1, n)},
        )

    def step(s, carry):
        @pl.when(s < chunks)
        def _():
            g, r = lax.div(s, parts), lax.rem(s, parts)

            @pl.when(r == 0)
            def _():
                complete(g)

            @pl.when(jnp.logical_and(r == parts // 2, g < n - 1))
            def _():
                forward(g + 1)

            part[s] = jnp.dot(img_ref[r], wown[g], preferred_element_type=jnp.float32)

        kp = s - SKEW * z

        @pl.when(jnp.logical_and(kp >= 0, kp < chunks))
        def _():
            @pl.when(z > 0)
            def _():
                right_copy(kp).wait_recv()

            @pl.when(z < n - 1)
            def _():
                pre_out[kp] = (part[kp] + pre_in[kp].astype(jnp.float32)).astype(jnp.bfloat16)
                right_copy(kp).start()

        ks = s - SKEW * (n - 1 - z)

        @pl.when(jnp.logical_and(ks >= 0, ks < chunks))
        def _():
            @pl.when(z < n - 1)
            def _():
                left_copy(ks).wait_recv()

            @pl.when(z > 0)
            def _():
                suf_out[ks] = (part[ks] + suf_in[ks].astype(jnp.float32)).astype(jnp.bfloat16)
                left_copy(ks).start()

        kf = s - SKEW * jnp.maximum(z, n - 1 - z)

        @pl.when(jnp.logical_and(kf >= 0, kf < chunks))
        def _():
            g, r = lax.div(kf, parts), lax.rem(kf, parts)
            value = (
                part[kf] + pre_in[kf].astype(jnp.float32) + suf_in[kf].astype(jnp.float32)
            )
            part[kf] = value

            @pl.when(r == 0)
            def _():
                shift[g] = jnp.sum(value, axis=0, keepdims=True) / height
                acc1[g] = jnp.zeros_like(acc1[g])
                acc2[g] = jnp.zeros_like(acc2[g])

            moved = value - shift[g]
            acc1[g] += jnp.sum(moved, axis=0, keepdims=True)
            acc2[g] += jnp.sum(moved * moved, axis=0, keepdims=True)

        return carry

    lax.fori_loop(0, chunks + SKEW * (n - 1), step, 0)

    local = height * parts
    extra = acc1[...] / local
    stat_in[b, :, 0:1, :] = shift[...] + extra
    stat_in[b, :, 1:2, :] = acc2[...] - acc1[...] * extra
    share_stats(nb, b, stat_in, st_send, st_recv)
    for off in range(1, n):
        g = lax.rem(z + off, n)
        remote(gb_ref, gb_in.at[g], gb_send.at[off], gb_recv.at[g], {"chan": g}).wait()
    mean, var = combine(stat_in[...], local)
    scale = gb_in[:, 0:1, :] / jnp.sqrt(var + eps)
    bias = gb_in[:, 1:2, :]
    width = part.shape[2]

    def finish(r, carry):
        for g in range(n):
            value = (part[g * parts + r] - mean[g]) * scale[g] + bias[g]
            out_ref[r, :, g * width : (g + 1) * width] = jnp.maximum(value, 0.0).astype(
                jnp.bfloat16
            )
        return carry

    lax.fori_loop(0, parts, finish, 0)

    for off in range(1, n):
        to = lax.rem(z + off, n)
        src = w_ref.at[pl.ds(pl.multiple_of(to * depth + b * strip, 16), strip), :]
        remote(
            src, wown.at[z, rows_of(b), :], w1_send.at[off], w1_recv.at[z], {"chan": to}
        ).wait_send()
        g = to
        for hop in range(1, half):
            peer = lax.rem(b + 2 * hop, nb)
            strip_copy(g, b, w2_send.at[g, hop], w2_recv.at[g, b], {"batch": peer}).wait_send()
        for hop in range(half):
            peer = lax.rem(b + 2 * hop, nb)
            strip_copy(
                g, peer, w3_send.at[g, hop], w3_recv.at[g, peer], {"batch": partner}
            ).wait_send()

    def drain(k, carry):
        @pl.when(z < n - 1)
        def _():
            right_copy(k).wait_send()

        @pl.when(z > 0)
        def _():
            left_copy(k).wait_send()

        return carry

    lax.fori_loop(0, chunks, drain, 0)


def third_kernel(
    n, nb, imgs, one_ref, sw_ref, gb_ref, w_ref, gain_ref, out_ref, norm_ref,
    pad, act, shift, acc1, acc2, stat2, affine, stat3,
    right_send, left_send, recv, s2_send, s2_recv, af_send, af_recv, s3_send, s3_recv,
):
    z, b = lax.axis_index("chan"), lax.axis_index("batch")
    side, height, mid = one_ref.shape
    parts, tall, width = act.shape[1:]
    join = side // parts
    local = parts * tall
    pad[:, 0] = jnp.zeros_like(pad[:, 0])
    pad[:, side + 1] = jnp.zeros_like(pad[:, 0])

    def spread(r, carry):
        row = one_ref[r]
        wide = row.astype(jnp.float32)
        edge = jnp.zeros((imgs, mid), jnp.float32)
        pad[1, r + 1] = row
        pad[0, r + 1] = jnp.concatenate([edge, wide[:-imgs]], axis=0).astype(jnp.bfloat16)
        pad[2, r + 1] = jnp.concatenate([wide[imgs:], edge], axis=0).astype(jnp.bfloat16)
        return carry

    lax.fori_loop(0, side, spread, 0)
    acc1[...] = jnp.zeros_like(acc1)
    acc2[...] = jnp.zeros_like(acc2)
    greet(n, nb, z, b)

    def right_copy(g, r):
        ref = act.at[g, r]
        return remote(
            ref, ref, right_send.at[g, r], recv.at[g, r], {"chan": lax.rem(z + 1, n)}
        )

    def left_copy(g, r):
        ref = act.at[g, r]
        return remote(
            ref, ref, left_send.at[g, r], recv.at[g, r], {"chan": lax.rem(z + n - 1, n)}
        )

    def rows_of(g):
        return pl.ds(pl.multiple_of(g * width, 128), width)

    def convolve(r, carry):
        total = jnp.zeros((tall, width), jnp.float32)
        for row_tap in range(3):
            for col_tap in range(3):
                window = pad[col_tap, pl.ds(r * join + row_tap, join)].reshape(tall, mid)
                total = total + jnp.dot(
                    window, sw_ref[row_tap, col_tap], preferred_element_type=jnp.float32
                )

        @pl.when(r == 0)
        def _():
            shift[...] = jnp.sum(total, axis=0, keepdims=True) / tall

        moved = total - shift[...]
        acc1[...] += jnp.sum(moved, axis=0, keepdims=True)
        acc2[...] += jnp.sum(moved * moved, axis=0, keepdims=True)
        act[z, r] = moved.astype(jnp.bfloat16)

        @pl.when(z < n - 1)
        def _():
            right_copy(z, r).start()

        @pl.when(z > 0)
        def _():
            left_copy(z, r).start()

        return carry

    lax.fori_loop(0, parts, convolve, 0)
    extra = acc1[...] / local
    stat2[b, 0:1, :] = shift[...] + extra
    stat2[b, 1:2, :] = acc2[...] - acc1[...] * extra
    share_stats(nb, b, stat2, s2_send, s2_recv)
    mean, var = combine(stat2[...], local)
    scale = gb_ref[0:1, :] / jnp.sqrt(var + eps)
    affine[z, 0:1, :] = scale
    affine[z, 1:2, :] = (shift[...] - mean) * scale + gb_ref[1:2, :]

    def affine_copy(off, slot):
        to = lax.rem(z + off, n)
        return remote(
            affine.at[z], affine.at[slot], af_send.at[off], af_recv.at[slot], {"chan": to}
        )

    for off in range(1, n):
        affine_copy(off, z).start()
    for off in range(1, n):
        affine_copy(off, lax.rem(z + off, n)).wait()

    def product(g, r):
        value = act[g, r].astype(jnp.float32) * affine[g, 0:1, :] + affine[g, 1:2, :]
        return jnp.dot(
            jnp.maximum(value, 0.0).astype(jnp.bfloat16),
            w_ref[rows_of(g), :],
            preferred_element_type=jnp.float32,
        )

    def relay(s, carry):
        d, r = lax.div(s, parts) + 1, lax.rem(s, parts)
        g, h = z - d, z + d

        @pl.when(g >= 0)
        def _():
            right_copy(g, r).wait_recv()

            @pl.when(z < n - 1)
            def _():
                right_copy(g, r).start()

        @pl.when(h < n)
        def _():
            left_copy(h, r).wait_recv()

            @pl.when(z > 0)
            def _():
                left_copy(h, r).start()

        @pl.when(d == 1)
        def _():
            out_ref[r] = product(z, r)

        @pl.when(g >= 0)
        def _():
            out_ref[r] += product(g, r)

        @pl.when(h < n)
        def _():
            out_ref[r] += product(h, r)

        return carry

    lax.fori_loop(0, parts * (n - 1), relay, 0)

    base = jnp.sum(out_ref[0], axis=0, keepdims=True) / tall

    def add(r, carry):
        moved = out_ref[r] - base
        return (
            carry[0] + jnp.sum(moved, axis=0, keepdims=True),
            carry[1] + jnp.sum(moved * moved, axis=0, keepdims=True),
        )

    zero = jnp.zeros((1, out_ref.shape[2]), jnp.float32)
    one3, two3 = lax.fori_loop(0, parts, add, (zero, zero))
    extra3 = one3 / local
    stat3[b, 0:1, :] = base + extra3
    stat3[b, 1:2, :] = two3 - one3 * extra3
    share_stats(nb, b, stat3, s3_send, s3_recv)
    mean3, var3 = combine(stat3[...], local)
    norm_ref[0:1, :] = mean3
    norm_ref[1:2, :] = gain_ref[...] / jnp.sqrt(var3 + eps)

    def drain(s, carry):
        g, r = lax.div(s, parts), lax.rem(s, parts)

        @pl.when(jnp.logical_and(z < n - 1, g <= z))
        def _():
            right_copy(g, r).wait_send()

        @pl.when(jnp.logical_and(z > 0, g >= z))
        def _():
            left_copy(g, r).wait_send()

        return carry

    lax.fori_loop(0, n * parts, drain, 0)


def body(
    images,
    reduce_weight,
    reduce_gain,
    reduce_bias,
    spatial_weight,
    spatial_gain,
    spatial_bias,
    expand_weight,
    expand_gain,
    expand_bias,
):
    imgs, side = (images.shape[0], images.shape[1])
    n, nb = lax.axis_size("chan"), lax.axis_size("batch")
    mid_local = reduce_weight.shape[1]
    mid = mid_local * n
    depth = images.shape[3]
    out_local = expand_weight.shape[1]
    parts, height = side, side * imgs
    chunks = n * parts
    dma, f32, bf16 = pltpu.SemaphoreType.DMA, jnp.float32, jnp.bfloat16
    vmem = pl.BlockSpec(memory_space=pltpu.VMEM)
    flat = images.transpose(1, 2, 0, 3).reshape(parts, height, depth)
    act_one = pl.pallas_call(
        functools.partial(first_kernel, n, nb, parts),
        out_shape=jax.ShapeDtypeStruct((parts, height, mid), bf16),
        in_specs=[vmem] * 3,
        out_specs=vmem,
        scratch_shapes=[
            pltpu.VMEM((n, depth, mid_local), bf16),
            pltpu.VMEM((chunks, height, mid_local), f32),
        ]
        + [pltpu.VMEM((chunks, height, mid_local), bf16)] * 4
        + [pltpu.VMEM((n, 2, mid_local), f32)]
        + [pltpu.VMEM((n, 1, mid_local), f32)] * 3
        + [pltpu.VMEM((nb, n, 2, mid_local), f32)]
        + [dma((n,)), dma((n,)), dma((n, nb // 2)), dma((n, nb)), dma((n, nb // 2)), dma((n, nb))]
        + [dma((n,)), dma((n,))]
        + [dma((chunks,))] * 4
        + [dma((nb,)), dma((nb,))],
        compiler_params=pltpu.CompilerParams(
            collective_id=0, has_side_effects=True, vmem_limit_bytes=LIMIT
        ),
        name="first",
    )(flat, reduce_weight, jnp.stack([reduce_gain, reduce_bias]))
    join = 2 if side % 2 == 0 else 1
    pieces, tall = side // join, height * join
    third, norm = pl.pallas_call(
        functools.partial(third_kernel, n, nb, imgs),
        out_shape=(
            jax.ShapeDtypeStruct((pieces, tall, out_local), f32),
            jax.ShapeDtypeStruct((2, out_local), f32),
        ),
        in_specs=[vmem] * 5,
        out_specs=(vmem, vmem),
        scratch_shapes=[
            pltpu.VMEM((3, side + 2, height, mid), bf16),
            pltpu.VMEM((n, pieces, tall, mid_local), bf16),
        ]
        + [pltpu.VMEM((1, mid_local), f32)] * 3
        + [
            pltpu.VMEM((nb, 2, mid_local), f32),
            pltpu.VMEM((n, 2, mid_local), f32),
            pltpu.VMEM((nb, 2, out_local), f32),
        ]
        + [dma((n, pieces))] * 3
        + [dma((nb,))] * 2
        + [dma((n,))] * 2
        + [dma((nb,))] * 2,
        compiler_params=pltpu.CompilerParams(
            collective_id=1, has_side_effects=True, vmem_limit_bytes=LIMIT
        ),
        name="third",
    )(
        act_one,
        spatial_weight,
        jnp.stack([spatial_gain, spatial_bias]),
        expand_weight,
        expand_gain[None, :],
    )
    third = third.reshape(side, height, out_local)
    normed = (third - norm[0]) * norm[1] + expand_bias
    out = jnp.maximum(normed + flat.astype(f32), 0.0).astype(bf16)
    return out.reshape(side, side, imgs, out_local).transpose(2, 0, 1, 3)


def solution(mesh):
    in_specs = (
        P("batch", None, None, "chan"),
        P(None, "chan"),
        P("chan"),
        P("chan"),
        P(None, None, None, "chan"),
        P("chan"),
        P("chan"),
        P(None, "chan"),
        P("chan"),
        P("chan"),
    )
    out_specs = P("batch", None, None, "chan")
    return jax.shard_map(body, mesh=mesh, in_specs=in_specs, out_specs=out_specs, check_vma=False)
```

```python
import functools

import jax
import jax.numpy as jnp
from jax import lax
from jax.experimental import pallas as pl
from jax.experimental.pallas import tpu as pltpu
from jax.sharding import PartitionSpec as P

eps = 0.001
MESH = pl.DeviceIdType.MESH
LIMIT = 63 * 1024 * 1024
SKEW = 3


def remote(src, dst, send, recv, device):
    return pltpu.make_async_remote_copy(
        src_ref=src, dst_ref=dst, send_sem=send, recv_sem=recv,
        device_id=device, device_id_type=MESH,
    )


def greet(n, nb, z, b):
    barrier = pltpu.get_barrier_semaphore()
    for off in range(1, n):
        pl.semaphore_signal(
            barrier, inc=1, device_id={"chan": lax.rem(z + off, n)}, device_id_type=MESH
        )
    for off in range(1, nb):
        pl.semaphore_signal(
            barrier, inc=1, device_id={"batch": lax.rem(b + off, nb)}, device_id_type=MESH
        )
    pl.semaphore_wait(barrier, n + nb - 2)


def share_stats(nb, b, stat_in, send, recv):
    for off in range(1, nb):
        peer = lax.rem(b + off, nb)
        remote(
            stat_in.at[b], stat_in.at[b], send.at[off], recv.at[b], {"batch": peer}
        ).start()
    for off in range(1, nb):
        peer = lax.rem(b + off, nb)
        remote(
            stat_in.at[b], stat_in.at[peer], send.at[off], recv.at[peer], {"batch": peer}
        ).wait()


def combine(stats, local):
    nb = stats.shape[0]
    means = stats[..., 0:1, :]
    mean = jnp.sum(means, axis=0) / nb
    away = means - mean[None]
    spread = jnp.sum(stats[..., 1:2, :], axis=0) + local * jnp.sum(away * away, axis=0)
    return mean, spread / (local * nb)


def first_kernel(
    n, nb, parts, img_hbm, w_ref, gain_ref, bias_ref, out_ref,
    img_ref, img_sem, wown, part, pre_in, suf_in, pre_out, suf_out, gb_in, shift, acc1, acc2, stat_in,
    w1_send, w1_recv, w2_send, w2_recv, w3_send, w3_recv, gb_send, gb_recv,
    pre_send, pre_recv, suf_send, suf_recv, st_send, st_recv,
):
    z, b = lax.axis_index("chan"), lax.axis_index("batch")
    depth = img_ref.shape[2]
    height = img_ref.shape[1]
    strip = depth // nb
    half = nb // 2
    chunks = n * parts
    partner = b + 1 - 2 * lax.rem(b, 2)
    parity = lax.rem(b, 2)
    img_load = pltpu.make_async_copy(img_hbm, img_ref, img_sem)
    img_load.start()
    gb_in[z, 0:1, :] = gain_ref[...]
    gb_in[z, 1:2, :] = bias_ref[...]
    greet(n, nb, z, b)

    def rows_of(who):
        return pl.ds(pl.multiple_of(who * strip, 16), strip)

    for off in range(1, n):
        to = lax.rem(z + off, n)
        src = w_ref.at[pl.ds(pl.multiple_of(to * depth + b * strip, 16), strip), :]
        remote(
            src, wown.at[z, rows_of(b), :], w1_send.at[off], w1_recv.at[z], {"chan": to}
        ).start()
    for off in range(1, n):
        to = lax.rem(z + off, n)
        remote(gb_in.at[z], gb_in.at[z], gb_send.at[off], gb_recv.at[z], {"chan": to}).start()

    wown[z] = w_ref[pl.ds(pl.multiple_of(z * depth, 16), depth), :]

    @pl.when(z == 0)
    def _():
        pre_in[...] = jnp.zeros_like(pre_in)

    @pl.when(z == n - 1)
    def _():
        suf_in[...] = jnp.zeros_like(suf_in)

    def strip_copy(g, who, send, recv, device):
        ref = wown.at[g, rows_of(who), :]
        return remote(ref, ref, send, recv, device)

    for g in range(n):

        @pl.when(z != g)
        def _():
            strip_copy(g, b, w1_send.at[0], w1_recv.at[g], {"chan": g}).wait_recv()
            for hop in range(1, half):
                peer = lax.rem(b + 2 * hop, nb)
                strip_copy(g, b, w2_send.at[g, hop], w2_recv.at[g, b], {"batch": peer}).start()
            strip_copy(g, b, w3_send.at[g, 0], w3_recv.at[g, b], {"batch": partner}).start()

    def forward(g):
        @pl.when(z != g)
        def _():
            for hop in range(1, half):
                peer = lax.rem(b + 2 * hop, nb)
                strip_copy(
                    g, peer, w2_send.at[g, 0], w2_recv.at[g, peer], {"batch": peer}
                ).wait_recv()
                strip_copy(
                    g, peer, w3_send.at[g, hop], w3_recv.at[g, peer], {"batch": partner}
                ).start()

    def complete(g):
        @pl.when(z != g)
        def _():
            for hop in range(half):
                who = 2 * hop + 1 - parity
                strip_copy(
                    g, who, w3_send.at[g, 0], w3_recv.at[g, who], {"batch": partner}
                ).wait_recv()

    forward(0)
    img_load.wait()

    def right_copy(k):
        return remote(
            pre_out.at[k], pre_in.at[k], pre_send.at[k], pre_recv.at[k],
            {"chan": lax.rem(z + 1, n)},
        )

    def left_copy(k):
        return remote(
            suf_out.at[k], suf_in.at[k], suf_send.at[k], suf_recv.at[k],
            {"chan": lax.rem(z + n - 1, n)},
        )

    def step(s, carry):
        @pl.when(s < chunks)
        def _():
            g, r = lax.div(s, parts), lax.rem(s, parts)

            @pl.when(r == 0)
            def _():
                complete(g)

            @pl.when(jnp.logical_and(r == parts // 2, g < n - 1))
            def _():
                forward(g + 1)

            part[s] = jnp.dot(img_ref[r], wown[g], preferred_element_type=jnp.float32)

        kp = s - SKEW * z

        @pl.when(jnp.logical_and(kp >= 0, kp < chunks))
        def _():
            @pl.when(z > 0)
            def _():
                right_copy(kp).wait_recv()

            @pl.when(z < n - 1)
            def _():
                pre_out[kp] = (part[kp] + pre_in[kp].astype(jnp.float32)).astype(jnp.bfloat16)
                right_copy(kp).start()

        ks = s - SKEW * (n - 1 - z)

        @pl.when(jnp.logical_and(ks >= 0, ks < chunks))
        def _():
            @pl.when(z < n - 1)
            def _():
                left_copy(ks).wait_recv()

            @pl.when(z > 0)
            def _():
                suf_out[ks] = (part[ks] + suf_in[ks].astype(jnp.float32)).astype(jnp.bfloat16)
                left_copy(ks).start()

        kf = s - SKEW * jnp.maximum(z, n - 1 - z)

        @pl.when(jnp.logical_and(kf >= 0, kf < chunks))
        def _():
            g, r = lax.div(kf, parts), lax.rem(kf, parts)
            value = (
                part[kf] + pre_in[kf].astype(jnp.float32) + suf_in[kf].astype(jnp.float32)
            )
            part[kf] = value

            @pl.when(r == 0)
            def _():
                shift[g] = jnp.sum(value, axis=0, keepdims=True) / height
                acc1[g] = jnp.zeros_like(acc1[g])
                acc2[g] = jnp.zeros_like(acc2[g])

            moved = value - shift[g]
            acc1[g] += jnp.sum(moved, axis=0, keepdims=True)
            acc2[g] += jnp.sum(moved * moved, axis=0, keepdims=True)

        return carry

    lax.fori_loop(0, chunks + SKEW * (n - 1), step, 0)

    local = height * parts
    extra = acc1[...] / local
    stat_in[b, :, 0:1, :] = shift[...] + extra
    stat_in[b, :, 1:2, :] = acc2[...] - acc1[...] * extra
    share_stats(nb, b, stat_in, st_send, st_recv)
    for off in range(1, n):
        g = lax.rem(z + off, n)
        remote(gb_in.at[z], gb_in.at[g], gb_send.at[off], gb_recv.at[g], {"chan": g}).wait()
    mean, var = combine(stat_in[...], local)
    scale = gb_in[:, 0:1, :] / jnp.sqrt(var + eps)
    bias = gb_in[:, 1:2, :]
    width = part.shape[2]

    def finish(r, carry):
        for g in range(n):
            value = (part[g * parts + r] - mean[g]) * scale[g] + bias[g]
            out_ref[r, :, g * width : (g + 1) * width] = jnp.maximum(value, 0.0).astype(
                jnp.bfloat16
            )
        return carry

    lax.fori_loop(0, parts, finish, 0)

    for off in range(1, n):
        to = lax.rem(z + off, n)
        src = w_ref.at[pl.ds(pl.multiple_of(to * depth + b * strip, 16), strip), :]
        remote(
            src, wown.at[z, rows_of(b), :], w1_send.at[off], w1_recv.at[z], {"chan": to}
        ).wait_send()
        g = to
        for hop in range(1, half):
            peer = lax.rem(b + 2 * hop, nb)
            strip_copy(g, b, w2_send.at[g, hop], w2_recv.at[g, b], {"batch": peer}).wait_send()
        for hop in range(half):
            peer = lax.rem(b + 2 * hop, nb)
            strip_copy(
                g, peer, w3_send.at[g, hop], w3_recv.at[g, peer], {"batch": partner}
            ).wait_send()

    def drain(k, carry):
        @pl.when(z < n - 1)
        def _():
            right_copy(k).wait_send()

        @pl.when(z > 0)
        def _():
            left_copy(k).wait_send()

        return carry

    lax.fori_loop(0, chunks, drain, 0)


def third_kernel(
    n, nb, imgs, one_ref, sw_hbm, mid_gain, mid_bias, w_hbm, gain_ref, out_ref, mean_ref, scale_ref,
    sw_ref, w_ref, sw_sem, w_sem, pad, act, shift, acc1, acc2, stat2, affine, stat3,
    right_send, left_send, recv, s2_send, s2_recv, af_send, af_recv, s3_send, s3_recv,
):
    z, b = lax.axis_index("chan"), lax.axis_index("batch")
    side, height, mid = one_ref.shape
    parts, tall, width = act.shape[1:]
    join = side // parts
    local = parts * tall
    sw_load = pltpu.make_async_copy(sw_hbm, sw_ref, sw_sem)
    sw_load.start()
    w_load = pltpu.make_async_copy(w_hbm, w_ref, w_sem)
    w_load.start()
    pad[:, 0] = jnp.zeros_like(pad[:, 0])
    pad[:, side + 1] = jnp.zeros_like(pad[:, 0])

    def spread(r, carry):
        row = one_ref[r]
        wide = row.astype(jnp.float32)
        edge = jnp.zeros((imgs, mid), jnp.float32)
        pad[1, r + 1] = row
        pad[0, r + 1] = jnp.concatenate([edge, wide[:-imgs]], axis=0).astype(jnp.bfloat16)
        pad[2, r + 1] = jnp.concatenate([wide[imgs:], edge], axis=0).astype(jnp.bfloat16)
        return carry

    lax.fori_loop(0, side, spread, 0)
    acc1[...] = jnp.zeros_like(acc1)
    acc2[...] = jnp.zeros_like(acc2)
    greet(n, nb, z, b)
    sw_load.wait()
    w_load.wait()

    def right_copy(g, r):
        ref = act.at[g, r]
        return remote(
            ref, ref, right_send.at[g, r], recv.at[g, r], {"chan": lax.rem(z + 1, n)}
        )

    def left_copy(g, r):
        ref = act.at[g, r]
        return remote(
            ref, ref, left_send.at[g, r], recv.at[g, r], {"chan": lax.rem(z + n - 1, n)}
        )

    def rows_of(g):
        return pl.ds(pl.multiple_of(g * width, 128), width)

    def convolve(r, carry):
        total = jnp.zeros((tall, width), jnp.float32)
        for row_tap in range(3):
            for col_tap in range(3):
                window = pad[col_tap, pl.ds(r * join + row_tap, join)].reshape(tall, mid)
                total = total + jnp.dot(
                    window, sw_ref[row_tap, col_tap], preferred_element_type=jnp.float32
                )

        @pl.when(r == 0)
        def _():
            shift[...] = jnp.sum(total, axis=0, keepdims=True) / tall

        moved = total - shift[...]
        acc1[...] += jnp.sum(moved, axis=0, keepdims=True)
        acc2[...] += jnp.sum(moved * moved, axis=0, keepdims=True)
        act[z, r] = moved.astype(jnp.bfloat16)

        @pl.when(z < n - 1)
        def _():
            right_copy(z, r).start()

        @pl.when(z > 0)
        def _():
            left_copy(z, r).start()

        return carry

    lax.fori_loop(0, parts, convolve, 0)
    extra = acc1[...] / local
    stat2[b, 0:1, :] = shift[...] + extra
    stat2[b, 1:2, :] = acc2[...] - acc1[...] * extra
    share_stats(nb, b, stat2, s2_send, s2_recv)
    mean, var = combine(stat2[...], local)
    scale = mid_gain[...] / jnp.sqrt(var + eps)
    affine[z, 0:1, :] = scale
    affine[z, 1:2, :] = (shift[...] - mean) * scale + mid_bias[...]

    def affine_copy(off, slot):
        to = lax.rem(z + off, n)
        return remote(
            affine.at[z], affine.at[slot], af_send.at[off], af_recv.at[slot], {"chan": to}
        )

    for off in range(1, n):
        affine_copy(off, z).start()
    for off in range(1, n):
        affine_copy(off, lax.rem(z + off, n)).wait()

    def product(g, r):
        value = act[g, r].astype(jnp.float32) * affine[g, 0:1, :] + affine[g, 1:2, :]
        return jnp.dot(
            jnp.maximum(value, 0.0).astype(jnp.bfloat16),
            w_ref[rows_of(g), :],
            preferred_element_type=jnp.float32,
        )

    def relay(s, carry):
        d, r = lax.div(s, parts) + 1, lax.rem(s, parts)
        g, h = z - d, z + d

        @pl.when(g >= 0)
        def _():
            right_copy(g, r).wait_recv()

            @pl.when(z < n - 1)
            def _():
                right_copy(g, r).start()

        @pl.when(h < n)
        def _():
            left_copy(h, r).wait_recv()

            @pl.when(z > 0)
            def _():
                left_copy(h, r).start()

        @pl.when(d == 1)
        def _():
            out_ref[r] = product(z, r)

        @pl.when(g >= 0)
        def _():
            out_ref[r] += product(g, r)

        @pl.when(h < n)
        def _():
            out_ref[r] += product(h, r)

        return carry

    lax.fori_loop(0, parts * (n - 1), relay, 0)

    base = jnp.sum(out_ref[0], axis=0, keepdims=True) / tall

    def add(r, carry):
        moved = out_ref[r] - base
        return (
            carry[0] + jnp.sum(moved, axis=0, keepdims=True),
            carry[1] + jnp.sum(moved * moved, axis=0, keepdims=True),
        )

    zero = jnp.zeros((1, out_ref.shape[2]), jnp.float32)
    one3, two3 = lax.fori_loop(0, parts, add, (zero, zero))
    extra3 = one3 / local
    stat3[b, 0:1, :] = base + extra3
    stat3[b, 1:2, :] = two3 - one3 * extra3
    share_stats(nb, b, stat3, s3_send, s3_recv)
    mean3, var3 = combine(stat3[...], local)
    mean_ref[...] = mean3
    scale_ref[...] = gain_ref[...] / jnp.sqrt(var3 + eps)

    def drain(s, carry):
        g, r = lax.div(s, parts), lax.rem(s, parts)

        @pl.when(jnp.logical_and(z < n - 1, g <= z))
        def _():
            right_copy(g, r).wait_send()

        @pl.when(jnp.logical_and(z > 0, g >= z))
        def _():
            left_copy(g, r).wait_send()

        return carry

    lax.fori_loop(0, n * parts, drain, 0)


def body(
    images,
    reduce_weight,
    reduce_gain,
    reduce_bias,
    spatial_weight,
    spatial_gain,
    spatial_bias,
    expand_weight,
    expand_gain,
    expand_bias,
):
    imgs, side = (images.shape[0], images.shape[1])
    n, nb = lax.axis_size("chan"), lax.axis_size("batch")
    mid_local = reduce_weight.shape[1]
    mid = mid_local * n
    depth = images.shape[3]
    out_local = expand_weight.shape[1]
    parts, height = side, side * imgs
    chunks = n * parts
    dma, f32, bf16 = pltpu.SemaphoreType.DMA, jnp.float32, jnp.bfloat16
    vmem = pl.BlockSpec(memory_space=pltpu.VMEM)
    flat = images.transpose(1, 2, 0, 3).reshape(parts, height, depth)
    act_one = pl.pallas_call(
        functools.partial(first_kernel, n, nb, parts),
        out_shape=jax.ShapeDtypeStruct((parts, height, mid), bf16),
        in_specs=[pl.BlockSpec(memory_space=pl.ANY)] + [vmem] * 3,
        out_specs=vmem,
        scratch_shapes=[
            pltpu.VMEM((parts, height, depth), bf16),
            dma,
            pltpu.VMEM((n, depth, mid_local), bf16),
            pltpu.VMEM((chunks, height, mid_local), f32),
        ]
        + [pltpu.VMEM((chunks, height, mid_local), bf16)] * 4
        + [pltpu.VMEM((n, 2, mid_local), f32)]
        + [pltpu.VMEM((n, 1, mid_local), f32)] * 3
        + [pltpu.VMEM((nb, n, 2, mid_local), f32)]
        + [dma((n,)), dma((n,)), dma((n, nb // 2)), dma((n, nb)), dma((n, nb // 2)), dma((n, nb))]
        + [dma((n,)), dma((n,))]
        + [dma((chunks,))] * 4
        + [dma((nb,)), dma((nb,))],
        compiler_params=pltpu.CompilerParams(
            collective_id=0, has_side_effects=True, vmem_limit_bytes=LIMIT
        ),
        name="first",
    )(flat, reduce_weight, reduce_gain[None, :], reduce_bias[None, :])
    anywhere = pl.BlockSpec(memory_space=pl.ANY)
    join = 2 if side % 2 == 0 else 1
    pieces, tall = side // join, height * join
    third, mean, scale = pl.pallas_call(
        functools.partial(third_kernel, n, nb, imgs),
        out_shape=(
            jax.ShapeDtypeStruct((pieces, tall, out_local), f32),
            jax.ShapeDtypeStruct((1, out_local), f32),
            jax.ShapeDtypeStruct((1, out_local), f32),
        ),
        in_specs=[vmem, anywhere, vmem, vmem, anywhere, vmem],
        out_specs=(vmem, vmem, vmem),
        scratch_shapes=[
            pltpu.VMEM(spatial_weight.shape, bf16),
            pltpu.VMEM(expand_weight.shape, bf16),
            dma,
            dma,
            pltpu.VMEM((3, side + 2, height, mid), bf16),
            pltpu.VMEM((n, pieces, tall, mid_local), bf16),
        ]
        + [pltpu.VMEM((1, mid_local), f32)] * 3
        + [
            pltpu.VMEM((nb, 2, mid_local), f32),
            pltpu.VMEM((n, 2, mid_local), f32),
            pltpu.VMEM((nb, 2, out_local), f32),
        ]
        + [dma((n, pieces))] * 3
        + [dma((nb,))] * 2
        + [dma((n,))] * 2
        + [dma((nb,))] * 2,
        compiler_params=pltpu.CompilerParams(
            collective_id=1, has_side_effects=True, vmem_limit_bytes=LIMIT
        ),
        name="third",
    )(
        act_one,
        spatial_weight,
        spatial_gain[None, :],
        spatial_bias[None, :],
        expand_weight,
        expand_gain[None, :],
    )
    third = third.reshape(side, height, out_local)
    normed = (third - mean[0]) * scale[0] + expand_bias
    out = jnp.maximum(normed + flat.astype(f32), 0.0).astype(bf16)
    return out.reshape(side, side, imgs, out_local).transpose(2, 0, 1, 3)


def solution(mesh):
    in_specs = (
        P("batch", None, None, "chan"),
        P(None, "chan"),
        P("chan"),
        P("chan"),
        P(None, None, None, "chan"),
        P("chan"),
        P("chan"),
        P(None, "chan"),
        P("chan"),
        P("chan"),
    )
    out_specs = P("batch", None, None, "chan")
    return jax.shard_map(body, mesh=mesh, in_specs=in_specs, out_specs=out_specs, check_vma=False)
```
